32 devices in a mesh: lat: 4 (over y, x), lon: 4 (over z), ens: 2 (over core).
Axes of the slice: x: 2, y: 2, z: 4, core: 2. Of those that a mesh axis runs over, the one named last changes fastest.
Arguments:
- parameters: float32 [2, 128, 32, 512], P(None, 'ens', 'lat', 'lon'), may hold values from -1.2 to 1.2, as said below
- initial_height: float32 [32, 512], P('lat', 'lon'), may hold values from -6 to 6
- initial_speed: float32 [2, 32, 512], P(None, 'lat', 'lon'), may hold values from -4 to 4
- obs_slots: int32 [2, 16, 16, 8], P(None, ('lat', 'lon')), may hold values from -1 to 1023, as said below
- obs_values: float32 [2, 16, 16, 8], P(None, ('lat', 'lon')), may hold values from -6 to 6
- obs_precision: float32 [2, 16, 16, 8], P(None, ('lat', 'lon')), may hold values from 0 to 2, as said below
Outputs:
- calibrated: float32 [2, 128, 32, 512], P(None, 'ens', 'lat', 'lon')
The draws below stay inside these ranges and needn't reach their ends.
Inputs may be any that keep to these rules, and one draw needn't show every extreme that they name: `obs_slots`: for each iteration and owner, the live slots towards one receiver come first and name distinct cells of the owner's block (local index row * 128 + column); no cell is named twice by one owner in one iteration; in each iteration some receiving block has all 8 slots live from every owner. `obs_precision`: zero exactly where the matching slot of obs_slots (with receiver and owner swapped) is empty, 0.5 or more elsewhere. `parameters`: friction rates lie in 0.02 to 0.2, forcing in -1.2 to 1.2.
All inputs are finite; a program needn't handle non-finite values.
Results may differ from the reference program's by a relative error of at most 0.0003.
Values sent between devices are 32-bit elements; how exact they have to be, the bound alone decides.
A program may use at most 64 MiB of HBM per device.

```python
import jax
import jax.numpy as jnp
from jax import lax

CLAT = 8
CLON = 128
MEMBERS = 128
STEPS = 6
ITERS = 2
CAP = 8
NLAT = 32
NLON = 512
OWNERS = 16
N_LAT = 4
N_LON = 4


def live_counts(key):
    owners = N_LAT * N_LON
    base = jax.random.fold_in(key, 7)
    counts = jax.random.randint(base, (ITERS, owners, owners), CAP // 4, CAP + 1)
    full_dest = jax.random.randint(jax.random.fold_in(base, 1), (ITERS,), 0, owners)
    receivers = jnp.arange(owners)
    counts = jnp.where(receivers[None, None, :] == full_dest[:, None, None], CAP, counts)
    slot_ids = jnp.arange(CAP)
    return slot_ids[None, None, None, :] < counts[..., None]


def draw_obs_slots(key, part):
    owners = N_LAT * N_LON
    live = live_counts(key)
    subkeys = jax.random.split(jax.random.fold_in(key, 11), ITERS * owners)
    orders = jax.vmap(lambda sub: jax.random.permutation(sub, CLAT * CLON))(subkeys)
    chosen = orders[:, :owners * CAP].reshape(ITERS, owners, owners, CAP).astype(jnp.int32)
    return jnp.where(live, chosen, -1).astype(jnp.int32)


def draw_obs_precision(key, part):
    owners = N_LAT * N_LON
    live = jnp.transpose(live_counts(key), (0, 2, 1, 3))
    sub = jax.random.fold_in(key, 23)
    values = jnp.exp(jax.random.uniform(sub, (ITERS, owners, owners, CAP), jnp.float32, jnp.log(0.5), jnp.log(2.0)))
    return jnp.where(live, values, 0.0).astype(jnp.float32)


def draw_parameters(key, part):
    first = jax.random.fold_in(key, 31)
    second = jax.random.fold_in(key, 37)
    friction = jnp.exp(jax.random.uniform(first, (MEMBERS, NLAT, NLON), jnp.float32, jnp.log(0.02), jnp.log(0.2)))
    forcing = jnp.clip(0.3 * jax.random.normal(second, (MEMBERS, NLAT, NLON), jnp.float32), -1.2, 1.2)
    return jnp.stack([friction, forcing]).astype(jnp.float32)


def levels(rng, shape, pieces, smallest, top_value):
    def one(position, shards_of):
        heights = jax.random.uniform(jax.random.fold_in(jax.random.fold_in(rng, 6), position), (shards_of,), jnp.float32, smallest / len(pieces), top_value / len(pieces))
        return jnp.repeat(jnp.exp(heights), shape[position] // shards_of).reshape((-1,) + (1,) * (len(shape) - position - 1))

    loudness = one(*pieces[0])
    for cut in pieces[1:]:
        loudness = loudness * one(*cut)
    return loudness


def bell_draw(stream_key, dims, deviation, most, pieces=(), held_as=jnp.bfloat16):
    gain = levels(stream_key, dims, pieces, -0.22, 0.18) if pieces else 1.0
    entries = jax.random.normal(stream_key, dims, jnp.float32) * deviation * gain
    return jnp.minimum(jnp.maximum(entries, -most), most).astype(held_as)


def setup_inputs(seed: int = 0) -> dict:
    arg_keys = jax.random.split(jax.random.key(seed), 7)
    parameters = draw_parameters(jax.random.fold_in(arg_keys[6], 71), 0)
    initial_height = bell_draw(arg_keys[1], (NLAT, NLON), 1.0, 6.0, ((0, 4), (1, 4)), jnp.float32)
    initial_speed = bell_draw(arg_keys[2], (2, NLAT, NLON), 0.5, 4.0, ((1, 4), (2, 4)), jnp.float32)
    obs_slots = draw_obs_slots(jax.random.fold_in(arg_keys[6], 71), 0)
    obs_values = bell_draw(arg_keys[4], (ITERS, OWNERS, OWNERS, CAP), 1.0, 6.0, ((1, 16),), jnp.float32)
    obs_precision = draw_obs_precision(jax.random.fold_in(arg_keys[6], 71), 0)
    return dict(parameters=parameters, initial_height=initial_height, initial_speed=initial_speed, obs_slots=obs_slots, obs_values=obs_values, obs_precision=obs_precision)


depth_step = 0.7
gravity_step = 0.7
coriolis = 0.1

def pad_grid(field):
    wrapped = jnp.concatenate([field[..., -1:], field, field[..., :1]], axis=-1)
    widths = [(0, 0)] * (field.ndim - 2) + [(1, 1), (0, 0)]
    return jnp.pad(wrapped, widths)

def forward(parameters, initial_height, initial_speed):
    members = parameters.shape[1]
    height = jnp.broadcast_to(initial_height, (members,) + initial_height.shape)
    speeds = jnp.broadcast_to(initial_speed[:, None], (2, members) + initial_height.shape)
    friction = parameters[0]
    forcing = parameters[1]
    for substep in range(STEPS):
        padded = pad_grid(speeds)
        east_diff = padded[0, :, 1:-1, 2:] - padded[0, :, 1:-1, :-2]
        north_diff = padded[1, :, 2:, 1:-1] - padded[1, :, :-2, 1:-1]
        height = height - depth_step * (east_diff + north_diff) + forcing
        padded_height = pad_grid(height)
        slope_east = padded_height[:, 1:-1, 2:] - padded_height[:, 1:-1, :-2]
        slope_north = padded_height[:, 2:, 1:-1] - padded_height[:, :-2, 1:-1]
        eastward = (1.0 - friction) * speeds[0] - gravity_step * slope_east + coriolis * speeds[1]
        northward = (1.0 - friction) * speeds[1] - gravity_step * slope_north - coriolis * speeds[0]
        speeds = jnp.stack([eastward, northward])
    return height

def gram_terms(predicted, observed, precision):
    members = predicted.shape[1]
    centre = lax.optimization_barrier(jnp.mean(predicted, axis=1, keepdims=True))
    spread = predicted - centre
    weighted = spread * precision[:, None]
    misfit = observed[:, None] - predicted
    gram_part = jnp.dot(spread.T, weighted, precision=lax.Precision.HIGHEST) / members
    cross_part = jnp.dot(weighted.T, misfit, precision=lax.Precision.HIGHEST) / jnp.sqrt(jnp.float32(members))
    return (gram_part, cross_part)

def solve_weights(gram_part, cross_part):
    members = gram_part.shape[0]
    system = jnp.eye(members, dtype=jnp.float32) + gram_part
    factor = jnp.linalg.cholesky(system)
    weights = jax.scipy.linalg.cho_solve((factor, True), cross_part) / jnp.sqrt(jnp.float32(members))
    return weights - lax.optimization_barrier(jnp.mean(weights, axis=0, keepdims=True))

def reference(parameters, initial_height, initial_speed, obs_slots, obs_values, obs_precision):
    owners = N_LAT * N_LON
    members = parameters.shape[1]
    owner_ids = jnp.arange(owners, dtype=jnp.int32)[:, None, None]
    for iteration in range(ITERS):
        height = forward(parameters, initial_height, initial_speed)
        cells = obs_slots[iteration]
        local = jnp.maximum(cells, 0)
        grid_row = owner_ids // N_LON * CLAT + local // CLON
        grid_col = owner_ids % N_LON * CLON + local % CLON
        global_ids = jnp.transpose(grid_row * NLON + grid_col, (1, 0, 2)).reshape(-1).astype(jnp.int32)
        live = jnp.transpose(cells >= 0, (1, 0, 2)).reshape(-1)
        flattened = height.reshape(members, -1)
        predicted = jnp.take(flattened, global_ids, axis=1).T
        predicted = jnp.where(live[:, None], predicted, jnp.float32(0.0))
        observed = obs_values[iteration].reshape(-1)
        precision = obs_precision[iteration].reshape(-1)
        gram_part, cross_part = gram_terms(predicted, observed, precision)
        centred = solve_weights(gram_part, cross_part)
        stacked = parameters.reshape(2, members, -1)
        increment = jnp.einsum('pjc,jm->pmc', stacked, centred, precision=lax.Precision.HIGHEST)
        parameters = parameters + increment.reshape(parameters.shape)
    return parameters
```

```python
import math

import functools

import jax
import jax.numpy as jnp
from jax import lax
from jax.experimental import pallas as pl
from jax.experimental.pallas import tpu as pltpu
from jax.sharding import PartitionSpec as P

STEPS = 6
ITERS = 2


depth_step = 0.7
gravity_step = 0.7
coriolis = 0.1


def padded_2(value, sides, width, wrap):
    for axis, dim in sides:
        peers, length = (lax.axis_size(axis), value.shape[dim])
        up = [(i, (i + 1) % peers) for i in range(peers if wrap else peers - 1)]
        down = [(j, i) for i, j in up]
        last = lax.slice_in_dim(value, length - width, length, axis=dim)
        leading = lax.slice_in_dim(value, 0, width, axis=dim)
        before = lax.ppermute(last, axis, up)
        after = lax.ppermute(leading, axis, down)
        value = jnp.concatenate([before, value, after], axis=dim)
    return value


def wall_rows(padded):
    row_count = padded.shape[-2]
    position = lax.axis_index("lat")
    last_block = lax.axis_size("lat") - 1
    row_ids = lax.broadcasted_iota(jnp.int32, (row_count, 1), 0)
    lower_wall = jnp.logical_and(row_ids == 0, position == 0)
    upper_wall = jnp.logical_and(row_ids == row_count - 1, position == last_block)
    keep_rows = jnp.logical_not(jnp.logical_or(lower_wall, upper_wall))
    return padded * keep_rows.astype(padded.dtype)


def advance(height, speeds, friction, forcing):
    east_padded = padded_2(speeds[0], (("lon", 2),), 1, True)
    north_padded = padded_2(speeds[1], (("lat", 1),), 1, False)
    east_diff = east_padded[:, :, 2:] - east_padded[:, :, :-2]
    north_diff = north_padded[:, 2:, :] - north_padded[:, :-2, :]
    height = height - depth_step * (east_diff + north_diff) + forcing
    padded_height = padded_2(height, (("lat", 1), ("lon", 2)), 1, True)
    padded_height = wall_rows(padded_height)
    slope_east = padded_height[:, 1:-1, 2:] - padded_height[:, 1:-1, :-2]
    slope_north = padded_height[:, 2:, 1:-1] - padded_height[:, :-2, 1:-1]
    eastward = (1.0 - friction) * speeds[0] - gravity_step * slope_east + coriolis * speeds[1]
    northward = (1.0 - friction) * speeds[1] - gravity_step * slope_north - coriolis * speeds[0]
    return (height, jnp.stack([eastward, northward]))


def forward(parameters, initial_height, initial_speed):
    members = parameters.shape[1]
    height = jnp.broadcast_to(initial_height, (members,) + initial_height.shape)
    speeds = jnp.broadcast_to(initial_speed[:, None], (2, members) + initial_height.shape)
    for substep in range(STEPS):
        height, speeds = advance(height, speeds, parameters[0], parameters[1])
    return height


def predict(height, cells):
    flattened = height.reshape(height.shape[0], -1)
    wanted = cells.reshape(-1)
    picked = jnp.take(flattened, jnp.clip(wanted, 0, flattened.shape[1] - 1), axis=1)
    picked = jnp.where(wanted[None, :] >= 0, picked, jnp.float32(0.0))
    return picked.T.reshape(cells.shape[0], -1)


def gram_terms(predicted, observed, precision):
    members = predicted.shape[1]
    centre = jnp.mean(predicted, axis=1, keepdims=True)
    spread = predicted - centre
    weighted = spread * precision[:, None]
    misfit = observed[:, None] - predicted
    gram_part = jnp.dot(spread.T, weighted, precision=lax.Precision.HIGHEST) / members
    cross_part = jnp.dot(weighted.T, misfit, precision=lax.Precision.HIGHEST) / math.sqrt(members)
    return (gram_part, cross_part)


def solve_weights(gram_part, cross_part):
    members = gram_part.shape[0]
    system = jnp.eye(members, dtype=jnp.float32) + gram_part
    factor = jnp.linalg.cholesky(system)
    weights = jax.scipy.linalg.cho_solve((factor, True), cross_part) / math.sqrt(members)
    return weights - jnp.mean(weights, axis=0, keepdims=True)


def per_device_halo(parameters, initial_height, initial_speed, obs_slots, obs_values, obs_precision):
    owners = obs_slots.shape[2]
    slot_count = obs_slots.shape[3]
    members_here = parameters.shape[1]
    member_block = lax.axis_index("ens")
    owner_values, owner_precision = (
        lax.all_to_all(obs_values[:, 0], ("lat", "lon"), split_axis=1, concat_axis=1, tiled=True),
        lax.all_to_all(
            obs_precision[:, 0], ("lat", "lon"), split_axis=1, concat_axis=1, tiled=True
        ),
    )
    for iteration in range(ITERS):
        height = forward(parameters, initial_height, initial_speed)
        outgoing = predict(height, obs_slots[iteration, 0])
        received = outgoing
        observed = owner_values[iteration]
        precision = owner_precision[iteration]
        received = received.reshape(owners, slot_count, members_here)
        gathered = lax.all_gather(received, "ens", axis=2, tiled=True)
        members = gathered.shape[2]
        gram_part, cross_part = gram_terms(
            gathered.reshape(-1, members), observed.reshape(-1), precision.reshape(-1)
        )
        gram_part, cross_part = lax.psum((gram_part, cross_part), ("lat", "lon"))
        centred = solve_weights(gram_part, cross_part)
        local_weights = lax.dynamic_slice_in_dim(
            centred, member_block * members_here, members_here, 1
        )
        starting = jnp.zeros(
            (2, members_here, parameters.shape[2] * parameters.shape[3]), jnp.float32
        )
        pieces = lax.all_gather(parameters, "ens", axis=1, tiled=True)
        stacked = pieces.reshape(pieces.shape[0], pieces.shape[1], -1)
        increment = starting + jnp.einsum(
            "pjc,jm->pmc", stacked, local_weights, precision=lax.Precision.HIGHEST
        )
        parameters = parameters + increment.reshape(parameters.shape)
    return parameters


MESH = pl.DeviceIdType.MESH
VMEM = pltpu.VMEM


def east(field):
    width = field.shape[1]
    return pltpu.roll(field, width - 1, 1) - pltpu.roll(field, 1, 1)


def north(field, first_row, last_row):
    height = field.shape[0]
    after = jnp.where(last_row, 0.0, pltpu.roll(field, height - 1, 0))
    before = jnp.where(first_row, 0.0, pltpu.roll(field, 1, 0))
    return after - before


def run_member(height, speed_e, speed_n, friction, forcing):
    rows = lax.broadcasted_iota(jnp.int32, height.shape, 0)
    first_row, last_row = (rows == 0, rows == height.shape[0] - 1)
    keep = 1.0 - friction
    for substep in range(STEPS):
        flow = east(speed_e) + north(speed_n, first_row, last_row)
        height = height - depth_step * flow + forcing
        if substep < STEPS - 1:
            speed_e, speed_n = (
                keep * speed_e - gravity_step * east(height) + coriolis * speed_n,
                keep * speed_n
                - gravity_step * north(height, first_row, last_row)
                - coriolis * speed_e,
            )
    return height


def gather_kernel(iteration, n_lat, n_lon, n_ens, *refs):
    first = iteration == 0
    blocks = n_lat * n_lon
    if first:
        params, aux, gram, cross, other, full, got, send_a, recv_a = refs[:9]
        refs = refs[9:]
    else:
        params, full, gram, cross, other, got = refs[:6]
        refs = refs[6:]
    (field, outgoing, arrived, part, pieces, summed, total) = refs[:7]
    (send_p, recv_p, send_o, recv_o, send_y, recv_y, send_r, recv_r, send_t, recv_t) = refs[7:]
    lat, lon, ens = (lax.axis_index("lat"), lax.axis_index("lon"), lax.axis_index("ens"))
    me = lat * n_lon + lon
    here = ens * blocks + me
    everyone = blocks * n_ens
    mine = params.shape[1] // blocks
    rows, cols = params.shape[2:]

    def peer(block):
        return {"lat": block // n_lon, "lon": lax.rem(block, n_lon), "ens": ens}

    def anyone(flat):
        block = lax.rem(flat, blocks)
        return {"lat": block // n_lon, "lon": lax.rem(block, n_lon), "ens": flat // blocks}

    def each(count, body):
        def step(i, carry):
            body(i)
            return carry

        lax.fori_loop(1, count, step, 0)

    def send(src, dst, send_sem, recv_sem, device):
        return pltpu.make_async_remote_copy(
            src_ref=src,
            dst_ref=dst,
            send_sem=send_sem,
            recv_sem=recv_sem,
            device_id=device,
            device_id_type=MESH,
        )

    barrier = pltpu.get_barrier_semaphore()

    def greet(i):
        pl.semaphore_signal(
            barrier, inc=1, device_id=anyone(lax.rem(here + i, everyone)), device_id_type=MESH
        )

    each(everyone, greet)
    pl.semaphore_wait(barrier, everyone - 1)

    def param_copy(i):
        to = lax.rem(me + i, blocks)
        return send(
            params.at[:, pl.ds(to * mine, mine)], got.at[me], send_p.at[i], recv_p.at[i], peer(to)
        )

    def aux_copy(i):
        to = lax.rem(me + i, blocks)
        return send(aux, full.at[me], send_a.at[i], recv_a.at[i], peer(to))

    def start_params(i):
        if first:
            aux_copy(i).start()
        param_copy(i).start()

    each(blocks, start_params)

    def swap_copy(i):
        return send(
            params, other.at[0], send_o.at[0], recv_o.at[0], {"lat": lat, "lon": lon, "ens": 1 - ens}
        )

    swap_copy(0).start()
    got[me] = params[:, pl.ds(me * mine, mine)]
    if first:
        full[me] = aux[...]

    def end_params(i):
        if first:
            aux_copy(i).wait()
        param_copy(i).wait()

    each(blocks, end_params)

    def whole(pick):
        lines = []
        for a in range(n_lat):
            lines.append(jnp.concatenate([pick(a * n_lon + b) for b in range(n_lon)], axis=1))
        return jnp.concatenate(lines, axis=0)

    def member(j, carry):
        height = run_member(
            whole(lambda b: full[b, 0]),
            whole(lambda b: full[b, 1]),
            whole(lambda b: full[b, 2]),
            whole(lambda b: got[b, 0, j]),
            whole(lambda b: got[b, 1, j]),
        )
        for a in range(n_lat):
            for b in range(n_lon):
                field[a * n_lon + b, j] = height[
                    a * rows : (a + 1) * rows, b * cols : (b + 1) * cols
                ]
        return carry

    lax.fori_loop(0, mine, member, 0)

    row_ids = lax.broadcasted_iota(jnp.int32, (rows, cols), 0)

    def pick_block(b, carry):
        cells = full[b, 3][iteration : iteration + 1].astype(jnp.int32)
        cells = jnp.broadcast_to(cells, (rows, cols))
        lanes = jnp.bitwise_and(cells, cols - 1)
        hit = row_ids == jnp.right_shift(cells, cols.bit_length() - 1)
        found = jnp.zeros((rows, cols), jnp.float32)
        for j in range(mine):
            tile = jnp.take_along_axis(field[b, j], lanes, axis=1)
            value = jnp.sum(jnp.where(hit, tile, 0.0), axis=0, keepdims=True)
            found = jnp.where(row_ids == j, value, found)
        outgoing[b] = found
        return carry

    lax.fori_loop(0, blocks, pick_block, 0)

    def answer_copy(i):
        to = lax.rem(here + i, everyone)
        return send(
            outgoing.at[lax.rem(to, blocks)],
            arrived.at[here],
            send_y.at[i],
            recv_y.at[i],
            anyone(to),
        )

    each(everyone, lambda i: answer_copy(i).start())
    arrived[here] = outgoing[me]

    slots = full.shape[-1] // blocks
    heard = jnp.concatenate([full[b, 3] for b in range(blocks)], axis=0)
    kinds = full.shape[2]
    lane_ids = lax.broadcasted_iota(jnp.int32, heard.shape, 1)
    line_ids = lax.broadcasted_iota(jnp.int32, heard.shape, 0)
    square = (heard.shape[1], heard.shape[1])
    from_ids = lax.broadcasted_iota(jnp.int32, square, 0)
    to_ids = lax.broadcasted_iota(jnp.int32, square, 1)
    chosen = from_ids == me * slots + lax.rem(to_ids, slots)
    spread_out = jnp.dot(
        heard,
        chosen.astype(jnp.float32),
        precision=lax.Precision.HIGHEST,
        preferred_element_type=jnp.float32,
    )

    def of_kind(kind):
        wanted = line_ids == (lane_ids // slots) * kinds + kind
        return jnp.sum(jnp.where(wanted, spread_out, 0.0), axis=0, keepdims=True)

    observed = of_kind(2 + iteration)
    precision = of_kind(4 + iteration)

    each(everyone, lambda i: answer_copy(i).wait())

    predicted = jnp.concatenate([arrived[s][:mine] for s in range(everyone)], axis=0)
    members = predicted.shape[0]
    spread = predicted - jnp.sum(predicted, axis=0, keepdims=True) / members
    weighted = spread * precision
    is_gram = ens == 0
    right = jnp.where(is_gram, spread, observed - predicted)
    scale = jnp.where(is_gram, 1.0 / members, 1.0 / math.sqrt(members))
    product = lax.dot_general(
        weighted,
        right,
        (((1,), (1,)), ((), ())),
        precision=lax.Precision.HIGHEST,
        preferred_element_type=jnp.float32,
    )
    product = product * scale
    lines = members // blocks
    for b in range(blocks):
        part[b] = product[b * lines : (b + 1) * lines]

    def piece_copy(i):
        to = lax.rem(me + i, blocks)
        return send(part.at[to], pieces.at[me], send_r.at[i], recv_r.at[i], peer(to))

    each(blocks, lambda i: piece_copy(i).start())
    pieces[me] = part[me]
    each(blocks, lambda i: piece_copy(i).wait())
    line = pieces[0]
    for b in range(1, blocks):
        line = line + pieces[b]
    summed[...] = line

    def total_copy(i):
        to = lax.rem(here + i, everyone)
        return send(summed, total.at[here], send_t.at[i], recv_t.at[i], anyone(to))

    each(everyone, lambda i: total_copy(i).start())
    total[here] = line
    each(everyone, lambda i: total_copy(i).wait())
    for b in range(blocks):
        gram[b * lines : (b + 1) * lines, :] = total[b]
        cross[b * lines : (b + 1) * lines, :] = total[blocks + b]
    swap_copy(0).wait()


def gather_call(iteration, sizes, params, extra):
    n_lat, n_lon, n_ens = sizes
    blocks = n_lat * n_lon
    everyone = blocks * n_ens
    members_here, rows, cols = params.shape[1:]
    members = members_here * n_ens
    mine = members_here // blocks
    lines = members // blocks
    f32 = jnp.float32
    dma = pltpu.SemaphoreType.DMA
    first = iteration == 0
    outs = [
        jax.ShapeDtypeStruct((members, members), f32),
        jax.ShapeDtypeStruct((members, members), f32),
        jax.ShapeDtypeStruct((1,) + params.shape, f32),
    ]
    scratch = [
        VMEM((blocks, 2, mine, rows, cols), f32),
    ]
    if first:
        outs.append(jax.ShapeDtypeStruct((blocks,) + extra.shape, f32))
        scratch += [dma((blocks,)), dma((blocks,))]
    scratch += [
        VMEM((blocks, mine, rows, cols), f32),
        VMEM((blocks, rows, cols), f32),
        VMEM((everyone, rows, cols), f32),
        VMEM((blocks, lines, members), f32),
        VMEM((blocks, lines, members), f32),
        VMEM((lines, members), f32),
        VMEM((everyone, lines, members), f32),
        dma((blocks,)),
        dma((blocks,)),
        dma((1,)),
        dma((1,)),
        dma((everyone,)),
        dma((everyone,)),
        dma((blocks,)),
        dma((blocks,)),
        dma((everyone,)),
        dma((everyone,)),
    ]
    return pl.pallas_call(
        functools.partial(gather_kernel, iteration, n_lat, n_lon, n_ens),
        out_shape=outs,
        in_specs=[pl.BlockSpec(memory_space=VMEM)] * 2,
        out_specs=[pl.BlockSpec(memory_space=VMEM)] * len(outs),
        scratch_shapes=scratch,
        compiler_params=pltpu.CompilerParams(
            collective_id=iteration, has_side_effects=True, vmem_limit_bytes=40 * 2**20
        ),
    )(params, extra)


def with_rows(value, rows, start):
    end = start + rows.shape[0]
    pieces = [value[:start]] if start else []
    pieces.append(rows)
    if end < value.shape[0]:
        pieces.append(value[end:])
    return jnp.concatenate(pieces, axis=0)


def eliminate(left, right):
    size = left.shape[0]
    panel = 8
    row_ids = lax.broadcasted_iota(jnp.int32, (panel, size), 0)
    for start in range(0, size, panel):
        end = start + panel
        rows_left, rows_right = (left[start:end], right[start:end])
        columns = [
            jnp.broadcast_to(rows_left[:, start + k : start + k + 1], (panel, size))
            for k in range(panel)
        ]
        for k in range(panel):
            column = columns[k]
            inverse = 1.0 / column[k : k + 1]
            here = row_ids == k

            def reduce(value):
                pivot_row = value[k : k + 1] * inverse
                return jnp.where(here, pivot_row, value - column * pivot_row)

            rows_left, rows_right = (reduce(rows_left), reduce(rows_right))
            for later in range(k + 1, panel):
                columns[later] = reduce(columns[later])
        next_left, next_right = (left, right)
        for k in range(panel):
            column = left[:, start + k : start + k + 1]
            next_left = next_left - column * rows_left[k : k + 1]
            next_right = next_right - column * rows_right[k : k + 1]
        left = with_rows(next_left, rows_left, start)
        right = with_rows(next_right, rows_right, start)
    return right


def update_kernel(gram, cross, params, other, out):
    ens = lax.axis_index("ens")
    members = gram.shape[0]
    members_here = params.shape[1]
    ids = [lax.broadcasted_iota(jnp.int32, gram.shape, axis) for axis in (0, 1)]
    system = gram[...] + (ids[0] == ids[1]).astype(jnp.float32)
    weights = eliminate(system, cross[...]) / math.sqrt(members)
    centred = weights - jnp.sum(weights, axis=0, keepdims=True) / members
    turned = centred.T
    mine = jnp.where(ens == 0, turned[:members_here], turned[members_here:])
    mine = jnp.where(ens == 0, mine, pltpu.roll(mine, members_here, 1))
    for p in range(params.shape[0]):
        for r in range(params.shape[2]):
            local = params[p, :, r, :]
            stacked = jnp.concatenate([local, other[0, p, :, r, :]], axis=0)
            out[p, :, r, :] = local + jnp.dot(
                mine,
                stacked,
                precision=lax.Precision.HIGHEST,
                preferred_element_type=jnp.float32,
            )


def update_call(gram, cross, params, other):
    return pl.pallas_call(
        update_kernel,
        out_shape=jax.ShapeDtypeStruct(params.shape, jnp.float32),
        in_specs=[pl.BlockSpec(memory_space=VMEM)] * 4,
        out_specs=pl.BlockSpec(memory_space=VMEM),
        compiler_params=pltpu.CompilerParams(vmem_limit_bytes=40 * 2**20),
    )(gram, cross, params, other)


def per_device_members(
    sizes, parameters, initial_height, initial_speed, obs_slots, obs_values, obs_precision
):
    rows, cols = initial_height.shape
    lines = [
        v.reshape(ITERS, cols).astype(jnp.float32) for v in (obs_slots, obs_values, obs_precision)
    ]
    lines.append(jnp.zeros((rows - 3 * ITERS, cols), jnp.float32))
    aux = jnp.concatenate(
        [initial_height[None], initial_speed, jnp.concatenate(lines, axis=0)[None]], axis=0
    )
    gram, cross, other, full = gather_call(0, sizes, parameters, aux)
    parameters = update_call(gram, cross, parameters, other)
    for iteration in range(1, ITERS):
        gram, cross, other = gather_call(iteration, sizes, parameters, full)
        parameters = update_call(gram, cross, parameters, other)
    return parameters


def by_members(sizes, parameters, initial_height, initial_speed, obs_slots, *rest):
    n_lat, n_lon, n_ens = sizes
    blocks = n_lat * n_lon
    members_here, rows, cols = parameters.shape[1:]
    fits = (
        n_ens == 2
        and members_here % blocks == 0
        and members_here // blocks <= rows
        and rows == 8
        and members_here * n_ens == blocks * 8
        and cols == 128
        and obs_slots.shape[2] * obs_slots.shape[3] == cols
    )
    arguments = (parameters, initial_height, initial_speed, obs_slots) + rest
    if fits:
        return per_device_members(sizes, *arguments)
    return per_device_halo(*arguments)


def solution(mesh):
    placed = (
        P(None, "ens", "lat", "lon"),
        P("lat", "lon"),
        P(None, "lat", "lon"),
        P(None, ("lat", "lon"), None, None),
        P(None, ("lat", "lon"), None, None),
        P(None, ("lat", "lon"), None, None),
    )
    return jax.shard_map(
        functools.partial(by_members, tuple(mesh.shape[a] for a in ("lat", "lon", "ens"))),
        mesh=mesh,
        in_specs=placed,
        out_specs=P(None, "ens", "lat", "lon"),
        check_vma=False,
    )
```

```python
import math

import functools

import jax
import jax.numpy as jnp
from jax import lax
from jax.experimental import pallas as pl
from jax.experimental.pallas import tpu as pltpu
from jax.sharding import PartitionSpec as P

STEPS = 6
ITERS = 2


depth_step = 0.7
gravity_step = 0.7
coriolis = 0.1


def padded_2(value, sides, width, wrap):
    for axis, dim in sides:
        peers, length = (lax.axis_size(axis), value.shape[dim])
        up = [(i, (i + 1) % peers) for i in range(peers if wrap else peers - 1)]
        down = [(j, i) for i, j in up]
        last = lax.slice_in_dim(value, length - width, length, axis=dim)
        leading = lax.slice_in_dim(value, 0, width, axis=dim)
        before = lax.ppermute(last, axis, up)
        after = lax.ppermute(leading, axis, down)
        value = jnp.concatenate([before, value, after], axis=dim)
    return value


def wall_rows(padded):
    row_count = padded.shape[-2]
    position = lax.axis_index("lat")
    last_block = lax.axis_size("lat") - 1
    row_ids = lax.broadcasted_iota(jnp.int32, (row_count, 1), 0)
    lower_wall = jnp.logical_and(row_ids == 0, position == 0)
    upper_wall = jnp.logical_and(row_ids == row_count - 1, position == last_block)
    keep_rows = jnp.logical_not(jnp.logical_or(lower_wall, upper_wall))
    return padded * keep_rows.astype(padded.dtype)


def advance(height, speeds, friction, forcing):
    east_padded = padded_2(speeds[0], (("lon", 2),), 1, True)
    north_padded = padded_2(speeds[1], (("lat", 1),), 1, False)
    east_diff = east_padded[:, :, 2:] - east_padded[:, :, :-2]
    north_diff = north_padded[:, 2:, :] - north_padded[:, :-2, :]
    height = height - depth_step * (east_diff + north_diff) + forcing
    padded_height = padded_2(height, (("lat", 1), ("lon", 2)), 1, True)
    padded_height = wall_rows(padded_height)
    slope_east = padded_height[:, 1:-1, 2:] - padded_height[:, 1:-1, :-2]
    slope_north = padded_height[:, 2:, 1:-1] - padded_height[:, :-2, 1:-1]
    eastward = (1.0 - friction) * speeds[0] - gravity_step * slope_east + coriolis * speeds[1]
    northward = (1.0 - friction) * speeds[1] - gravity_step * slope_north - coriolis * speeds[0]
    return (height, jnp.stack([eastward, northward]))


def forward(parameters, initial_height, initial_speed):
    members = parameters.shape[1]
    height = jnp.broadcast_to(initial_height, (members,) + initial_height.shape)
    speeds = jnp.broadcast_to(initial_speed[:, None], (2, members) + initial_height.shape)
    for substep in range(STEPS):
        height, speeds = advance(height, speeds, parameters[0], parameters[1])
    return height


def predict(height, cells):
    flattened = height.reshape(height.shape[0], -1)
    wanted = cells.reshape(-1)
    picked = jnp.take(flattened, jnp.clip(wanted, 0, flattened.shape[1] - 1), axis=1)
    picked = jnp.where(wanted[None, :] >= 0, picked, jnp.float32(0.0))
    return picked.T.reshape(cells.shape[0], -1)


def gram_terms(predicted, observed, precision):
    members = predicted.shape[1]
    centre = jnp.mean(predicted, axis=1, keepdims=True)
    spread = predicted - centre
    weighted = spread * precision[:, None]
    misfit = observed[:, None] - predicted
    gram_part = jnp.dot(spread.T, weighted, precision=lax.Precision.HIGHEST) / members
    cross_part = jnp.dot(weighted.T, misfit, precision=lax.Precision.HIGHEST) / math.sqrt(members)
    return (gram_part, cross_part)


def solve_weights(gram_part, cross_part):
    members = gram_part.shape[0]
    system = jnp.eye(members, dtype=jnp.float32) + gram_part
    factor = jnp.linalg.cholesky(system)
    weights = jax.scipy.linalg.cho_solve((factor, True), cross_part) / math.sqrt(members)
    return weights - jnp.mean(weights, axis=0, keepdims=True)


def per_device_halo(parameters, initial_height, initial_speed, obs_slots, obs_values, obs_precision):
    owners = obs_slots.shape[2]
    slot_count = obs_slots.shape[3]
    members_here = parameters.shape[1]
    member_block = lax.axis_index("ens")
    owner_values, owner_precision = (
        lax.all_to_all(obs_values[:, 0], ("lat", "lon"), split_axis=1, concat_axis=1, tiled=True),
        lax.all_to_all(
            obs_precision[:, 0], ("lat", "lon"), split_axis=1, concat_axis=1, tiled=True
        ),
    )
    for iteration in range(ITERS):
        height = forward(parameters, initial_height, initial_speed)
        outgoing = predict(height, obs_slots[iteration, 0])
        received = outgoing
        observed = owner_values[iteration]
        precision = owner_precision[iteration]
        received = received.reshape(owners, slot_count, members_here)
        gathered = lax.all_gather(received, "ens", axis=2, tiled=True)
        members = gathered.shape[2]
        gram_part, cross_part = gram_terms(
            gathered.reshape(-1, members), observed.reshape(-1), precision.reshape(-1)
        )
        gram_part, cross_part = lax.psum((gram_part, cross_part), ("lat", "lon"))
        centred = solve_weights(gram_part, cross_part)
        local_weights = lax.dynamic_slice_in_dim(
            centred, member_block * members_here, members_here, 1
        )
        starting = jnp.zeros(
            (2, members_here, parameters.shape[2] * parameters.shape[3]), jnp.float32
        )
        pieces = lax.all_gather(parameters, "ens", axis=1, tiled=True)
        stacked = pieces.reshape(pieces.shape[0], pieces.shape[1], -1)
        increment = starting + jnp.einsum(
            "pjc,jm->pmc", stacked, local_weights, precision=lax.Precision.HIGHEST
        )
        parameters = parameters + increment.reshape(parameters.shape)
    return parameters


MESH = pl.DeviceIdType.MESH
VMEM = pltpu.VMEM


def east(field):
    width = field.shape[1]
    return pltpu.roll(field, width - 1, 1) - pltpu.roll(field, 1, 1)


def north(field, first_row, last_row):
    height = field.shape[0]
    after = jnp.where(last_row, 0.0, pltpu.roll(field, height - 1, 0))
    before = jnp.where(first_row, 0.0, pltpu.roll(field, 1, 0))
    return after - before


def run_member(height, speed_e, speed_n, friction, forcing):
    rows = lax.broadcasted_iota(jnp.int32, height.shape, 0)
    first_row, last_row = (rows == 0, rows == height.shape[0] - 1)
    keep = 1.0 - friction
    for substep in range(STEPS):
        flow = east(speed_e) + north(speed_n, first_row, last_row)
        height = height - depth_step * flow + forcing
        if substep < STEPS - 1:
            speed_e, speed_n = (
                keep * speed_e - gravity_step * east(height) + coriolis * speed_n,
                keep * speed_n
                - gravity_step * north(height, first_row, last_row)
                - coriolis * speed_e,
            )
    return height


def flat_line(block, width):
    depth, count = block.shape
    lanes = lax.broadcasted_iota(jnp.int32, (count, width), 1)
    slots = lax.broadcasted_iota(jnp.int32, (count, width), 0)
    spread_out = jnp.dot(
        block,
        (lax.rem(lanes, count) == slots).astype(jnp.float32),
        precision=lax.Precision.HIGHEST,
        preferred_element_type=jnp.float32,
    )
    owners = lax.broadcasted_iota(jnp.int32, (depth, width), 0)
    groups = lax.broadcasted_iota(jnp.int32, (depth, width), 1) // count
    return jnp.sum(jnp.where(owners == groups, spread_out, 0.0), axis=0, keepdims=True)


def gather_kernel(iteration, n_lat, n_lon, n_ens, *refs):
    first = iteration == 0
    blocks = n_lat * n_lon
    if first:
        params, start_height, start_speed, slots_in, values_in, precision_in = refs[:6]
        gram, cross, other, full, got, aux, send_a, recv_a, send_h, recv_h = refs[6:16]
        refs = refs[16:]
    else:
        params, full, gram, cross, other, got = refs[:6]
        refs = refs[6:]
    (outgoing, arrived, part, pieces, summed, total) = refs[:6]
    (send_p, recv_p, send_o, recv_o, send_y, recv_y, send_r, recv_r, send_t, recv_t) = refs[6:]
    lat, lon, ens = (lax.axis_index("lat"), lax.axis_index("lon"), lax.axis_index("ens"))
    me = lat * n_lon + lon
    here = ens * blocks + me
    everyone = blocks * n_ens
    mine = params.shape[1] // blocks
    rows, cols = params.shape[2:]

    def peer(block):
        return {"lat": block // n_lon, "lon": lax.rem(block, n_lon), "ens": ens}

    def anyone(flat):
        block = lax.rem(flat, blocks)
        return {"lat": block // n_lon, "lon": lax.rem(block, n_lon), "ens": flat // blocks}

    def each(count, body):
        def step(i, carry):
            body(i)
            return carry

        lax.fori_loop(1, count, step, 0)

    def send(src, dst, send_sem, recv_sem, device):
        return pltpu.make_async_remote_copy(
            src_ref=src,
            dst_ref=dst,
            send_sem=send_sem,
            recv_sem=recv_sem,
            device_id=device,
            device_id_type=MESH,
        )

    barrier = pltpu.get_barrier_semaphore()

    def greet(i):
        pl.semaphore_signal(
            barrier, inc=1, device_id=anyone(lax.rem(here + i, everyone)), device_id_type=MESH
        )

    each(everyone, greet)
    if first:
        lines = []
        for ref in (slots_in, values_in, precision_in):
            for t in range(ITERS):
                lines.append(flat_line(ref[t, 0].astype(jnp.float32), cols))
        lines.append(jnp.zeros((rows - len(lines), cols), jnp.float32))
        aux[0] = start_height[...]
        aux[1] = start_speed[0]
        aux[2] = start_speed[1]
        aux[3] = jnp.concatenate(lines, axis=0)
    pl.semaphore_wait(barrier, everyone - 1)

    partner = {"lat": lat, "lon": lon, "ens": 1 - ens}
    half = pl.ds(2 * ens, 2)

    def param_copy(j, i):
        to = lax.rem(me + i, blocks)
        return send(
            params.at[:, to * mine + j], got.at[me, j], send_p.at[j, i], recv_p.at[j, i], peer(to)
        )

    def aux_copy(i):
        to = lax.rem(me + i, blocks)
        return send(aux.at[half], full.at[me, half], send_a.at[i], recv_a.at[i], peer(to))

    def relay_copy():
        return send(full.at[:, half], full.at[:, half], send_h.at[0], recv_h.at[0], partner)

    if first:
        each(blocks, lambda i: aux_copy(i).start())
    for j in range(mine):
        each(blocks, functools.partial(lambda j, i: param_copy(j, i).start(), j))

    def swap_copy(i):
        return send(
            params, other.at[0], send_o.at[0], recv_o.at[0], partner
        )

    if first:
        full[me, half] = aux[half]
        each(blocks, lambda i: aux_copy(i).wait())
        relay_copy().start()
    swap_copy(0).start()
    for j in range(mine):
        got[me, j] = params[:, me * mine + j]
    if first:
        relay_copy().wait()

    def whole(pick):
        lines = []
        for a in range(n_lat):
            lines.append(jnp.concatenate([pick(a * n_lon + b) for b in range(n_lon)], axis=1))
        return jnp.concatenate(lines, axis=0)

    row_ids = lax.broadcasted_iota(jnp.int32, (rows, cols), 0)

    def member(j, carry):
        each(blocks, lambda i: param_copy(j, i).wait())
        height = run_member(
            whole(lambda b: full[b, 0]),
            whole(lambda b: full[b, 1]),
            whole(lambda b: full[b, 2]),
            whole(lambda b: got[b, j, 0]),
            whole(lambda b: got[b, j, 1]),
        )
        for b in range(blocks):
            cells = full[b, 3][iteration : iteration + 1].astype(jnp.int32)
            cells = jnp.broadcast_to(cells, (rows, cols))
            lanes = jnp.bitwise_and(cells, cols - 1)
            hit = row_ids == jnp.right_shift(cells, cols.bit_length() - 1)
            top, edge = ((b // n_lon) * rows, (b % n_lon) * cols)
            tile = height[top : top + rows, edge : edge + cols]
            found = jnp.where(hit, jnp.take_along_axis(tile, lanes, axis=1), 0.0)
            outgoing[b, pl.ds(j, 1)] = jnp.sum(found, axis=0, keepdims=True)
        return carry

    lax.fori_loop(0, mine, member, 0)

    def answer_copy(i):
        to = lax.rem(here + i, everyone)
        return send(
            outgoing.at[lax.rem(to, blocks)],
            arrived.at[here],
            send_y.at[i],
            recv_y.at[i],
            anyone(to),
        )

    each(everyone, lambda i: answer_copy(i).start())
    arrived[here] = outgoing[me]

    slots = full.shape[-1] // blocks
    heard = jnp.concatenate([full[b, 3] for b in range(blocks)], axis=0)
    kinds = full.shape[2]
    lane_ids = lax.broadcasted_iota(jnp.int32, heard.shape, 1)
    line_ids = lax.broadcasted_iota(jnp.int32, heard.shape, 0)
    square = (heard.shape[1], heard.shape[1])
    from_ids = lax.broadcasted_iota(jnp.int32, square, 0)
    to_ids = lax.broadcasted_iota(jnp.int32, square, 1)
    chosen = from_ids == me * slots + lax.rem(to_ids, slots)
    spread_out = jnp.dot(
        heard,
        chosen.astype(jnp.float32),
        precision=lax.Precision.HIGHEST,
        preferred_element_type=jnp.float32,
    )

    def of_kind(kind):
        wanted = line_ids == (lane_ids // slots) * kinds + kind
        return jnp.sum(jnp.where(wanted, spread_out, 0.0), axis=0, keepdims=True)

    observed = of_kind(2 + iteration)
    precision = of_kind(4 + iteration)

    each(everyone, lambda i: answer_copy(i).wait())

    predicted = jnp.concatenate([arrived[s] for s in range(everyone)], axis=0)
    members = predicted.shape[0]
    spread = predicted - jnp.sum(predicted, axis=0, keepdims=True) / members
    weighted = spread * precision
    is_gram = ens == 0
    right = jnp.where(is_gram, spread, observed - predicted)
    scale = jnp.where(is_gram, 1.0 / members, 1.0 / math.sqrt(members))
    product = lax.dot_general(
        weighted,
        right,
        (((1,), (1,)), ((), ())),
        precision=lax.Precision.HIGHEST,
        preferred_element_type=jnp.float32,
    )
    product = product * scale
    lines = members // blocks
    for b in range(blocks):
        part[b] = product[b * lines : (b + 1) * lines]

    def piece_copy(i):
        to = lax.rem(me + i, blocks)
        return send(part.at[to], pieces.at[me], send_r.at[i], recv_r.at[i], peer(to))

    each(blocks, lambda i: piece_copy(i).start())
    pieces[me] = part[me]
    each(blocks, lambda i: piece_copy(i).wait())
    line = pieces[0]
    for b in range(1, blocks):
        line = line + pieces[b]
    summed[...] = line

    def total_copy(i):
        to = lax.rem(here + i, everyone)
        return send(summed, total.at[here], send_t.at[i], recv_t.at[i], anyone(to))

    each(everyone, lambda i: total_copy(i).start())
    total[here] = line
    each(everyone, lambda i: total_copy(i).wait())
    for b in range(blocks):
        gram[b * lines : (b + 1) * lines, :] = total[b]
        cross[b * lines : (b + 1) * lines, :] = total[blocks + b]
    swap_copy(0).wait()


def gather_call(iteration, sizes, params, *extra):
    n_lat, n_lon, n_ens = sizes
    blocks = n_lat * n_lon
    everyone = blocks * n_ens
    members_here, rows, cols = params.shape[1:]
    members = members_here * n_ens
    mine = members_here // blocks
    lines = members // blocks
    f32 = jnp.float32
    dma = pltpu.SemaphoreType.DMA
    first = iteration == 0
    outs = [
        jax.ShapeDtypeStruct((members, members), f32),
        jax.ShapeDtypeStruct((members, members), f32),
        jax.ShapeDtypeStruct((1,) + params.shape, f32),
    ]
    scratch = [
        VMEM((blocks, mine, 2, rows, cols), f32),
    ]
    if first:
        outs.append(jax.ShapeDtypeStruct((blocks, 4, rows, cols), f32))
        scratch.append(VMEM((4, rows, cols), f32))
        scratch += [dma((blocks,)), dma((blocks,)), dma((1,)), dma((1,))]
    scratch += [
        VMEM((blocks, mine, cols), f32),
        VMEM((everyone, mine, cols), f32),
        VMEM((blocks, lines, members), f32),
        VMEM((blocks, lines, members), f32),
        VMEM((lines, members), f32),
        VMEM((everyone, lines, members), f32),
        dma((mine, blocks)),
        dma((mine, blocks)),
        dma((1,)),
        dma((1,)),
        dma((everyone,)),
        dma((everyone,)),
        dma((blocks,)),
        dma((blocks,)),
        dma((everyone,)),
        dma((everyone,)),
    ]
    return pl.pallas_call(
        functools.partial(gather_kernel, iteration, n_lat, n_lon, n_ens),
        out_shape=outs,
        in_specs=[pl.BlockSpec(memory_space=VMEM)] * (1 + len(extra)),
        out_specs=[pl.BlockSpec(memory_space=VMEM)] * len(outs),
        scratch_shapes=scratch,
        compiler_params=pltpu.CompilerParams(
            collective_id=iteration, has_side_effects=True, vmem_limit_bytes=40 * 2**20
        ),
    )(params, *extra)


def with_rows(value, rows, start):
    end = start + rows.shape[0]
    pieces = [value[:start]] if start else []
    pieces.append(rows)
    if end < value.shape[0]:
        pieces.append(value[end:])
    return jnp.concatenate(pieces, axis=0)


def eliminate(left, right):
    size = left.shape[0]
    panel = 8
    row_ids = lax.broadcasted_iota(jnp.int32, (panel, size), 0)
    for start in range(0, size, panel):
        end = start + panel
        rows_left, rows_right = (left[start:end], right[start:end])
        columns = [
            jnp.broadcast_to(rows_left[:, start + k : start + k + 1], (panel, size))
            for k in range(panel)
        ]
        for k in range(panel):
            column = columns[k]
            inverse = 1.0 / column[k : k + 1]
            here = row_ids == k

            def reduce(value):
                pivot_row = value[k : k + 1] * inverse
                return jnp.where(here, pivot_row, value - column * pivot_row)

            rows_left, rows_right = (reduce(rows_left), reduce(rows_right))
            for later in range(k + 1, panel):
                columns[later] = reduce(columns[later])
        next_left, next_right = (left, right)
        for k in range(panel):
            column = left[:, start + k : start + k + 1]
            next_left = next_left - column * rows_left[k : k + 1]
            next_right = next_right - column * rows_right[k : k + 1]
        left = with_rows(next_left, rows_left, start)
        right = with_rows(next_right, rows_right, start)
    return right


def update_kernel(gram, cross, params, other, out):
    ens = lax.axis_index("ens")
    members = gram.shape[0]
    members_here = params.shape[1]
    ids = [lax.broadcasted_iota(jnp.int32, gram.shape, axis) for axis in (0, 1)]
    system = gram[...] + (ids[0] == ids[1]).astype(jnp.float32)
    weights = eliminate(system, cross[...]) / math.sqrt(members)
    centred = weights - jnp.sum(weights, axis=0, keepdims=True) / members
    turned = centred.T
    mine = jnp.where(ens == 0, turned[:members_here], turned[members_here:])
    mine = jnp.where(ens == 0, mine, pltpu.roll(mine, members_here, 1))
    for p in range(params.shape[0]):
        for r in range(params.shape[2]):
            local = params[p, :, r, :]
            stacked = jnp.concatenate([local, other[0, p, :, r, :]], axis=0)
            out[p, :, r, :] = local + jnp.dot(
                mine,
                stacked,
                precision=lax.Precision.HIGHEST,
                preferred_element_type=jnp.float32,
            )


def update_call(gram, cross, params, other):
    return pl.pallas_call(
        update_kernel,
        out_shape=jax.ShapeDtypeStruct(params.shape, jnp.float32),
        in_specs=[pl.BlockSpec(memory_space=VMEM)] * 4,
        out_specs=pl.BlockSpec(memory_space=VMEM),
        compiler_params=pltpu.CompilerParams(vmem_limit_bytes=40 * 2**20),
    )(gram, cross, params, other)


def per_device_members(
    sizes, parameters, initial_height, initial_speed, obs_slots, obs_values, obs_precision
):
    observations = (obs_slots, obs_values, obs_precision)
    gram, cross, other, full = gather_call(
        0, sizes, parameters, initial_height, initial_speed, *observations
    )
    parameters = update_call(gram, cross, parameters, other)
    for iteration in range(1, ITERS):
        gram, cross, other = gather_call(iteration, sizes, parameters, full)
        parameters = update_call(gram, cross, parameters, other)
    return parameters


def by_members(sizes, parameters, initial_height, initial_speed, obs_slots, *rest):
    n_lat, n_lon, n_ens = sizes
    blocks = n_lat * n_lon
    members_here, rows, cols = parameters.shape[1:]
    fits = (
        n_ens == 2
        and members_here % blocks == 0
        and members_here // blocks <= rows
        and rows == 8
        and members_here * n_ens == blocks * 8
        and cols == 128
        and obs_slots.shape[2] * obs_slots.shape[3] == cols
    )
    arguments = (parameters, initial_height, initial_speed, obs_slots) + rest
    if fits:
        return per_device_members(sizes, *arguments)
    return per_device_halo(*arguments)


def solution(mesh):
    placed = (
        P(None, "ens", "lat", "lon"),
        P("lat", "lon"),
        P(None, "lat", "lon"),
        P(None, ("lat", "lon"), None, None),
        P(None, ("lat", "lon"), None, None),
        P(None, ("lat", "lon"), None, None),
    )
    return jax.shard_map(
        functools.partial(by_members, tuple(mesh.shape[a] for a in ("lat", "lon", "ens"))),
        mesh=mesh,
        in_specs=placed,
        out_specs=P(None, "ens", "lat", "lon"),
        check_vma=False,
    )
```

```python
import math

import functools

import jax
import jax.numpy as jnp
from jax import lax
from jax.experimental import pallas as pl
from jax.experimental.pallas import tpu as pltpu
from jax.sharding import PartitionSpec as P

STEPS = 6
ITERS = 2


depth_step = 0.7
gravity_step = 0.7
coriolis = 0.1


def padded_2(value, sides, width, wrap):
    for axis, dim in sides:
        peers, length = (lax.axis_size(axis), value.shape[dim])
        up = [(i, (i + 1) % peers) for i in range(peers if wrap else peers - 1)]
        down = [(j, i) for i, j in up]
        last = lax.slice_in_dim(value, length - width, length, axis=dim)
        leading = lax.slice_in_dim(value, 0, width, axis=dim)
        before = lax.ppermute(last, axis, up)
        after = lax.ppermute(leading, axis, down)
        value = jnp.concatenate([before, value, after], axis=dim)
    return value


def wall_rows(padded):
    row_count = padded.shape[-2]
    position = lax.axis_index("lat")
    last_block = lax.axis_size("lat") - 1
    row_ids = lax.broadcasted_iota(jnp.int32, (row_count, 1), 0)
    lower_wall = jnp.logical_and(row_ids == 0, position == 0)
    upper_wall = jnp.logical_and(row_ids == row_count - 1, position == last_block)
    keep_rows = jnp.logical_not(jnp.logical_or(lower_wall, upper_wall))
    return padded * keep_rows.astype(padded.dtype)


def advance(height, speeds, friction, forcing):
    east_padded = padded_2(speeds[0], (("lon", 2),), 1, True)
    north_padded = padded_2(speeds[1], (("lat", 1),), 1, False)
    east_diff = east_padded[:, :, 2:] - east_padded[:, :, :-2]
    north_diff = north_padded[:, 2:, :] - north_padded[:, :-2, :]
    height = height - depth_step * (east_diff + north_diff) + forcing
    padded_height = padded_2(height, (("lat", 1), ("lon", 2)), 1, True)
    padded_height = wall_rows(padded_height)
    slope_east = padded_height[:, 1:-1, 2:] - padded_height[:, 1:-1, :-2]
    slope_north = padded_height[:, 2:, 1:-1] - padded_height[:, :-2, 1:-1]
    eastward = (1.0 - friction) * speeds[0] - gravity_step * slope_east + coriolis * speeds[1]
    northward = (1.0 - friction) * speeds[1] - gravity_step * slope_north - coriolis * speeds[0]
    return (height, jnp.stack([eastward, northward]))


def forward(parameters, initial_height, initial_speed):
    members = parameters.shape[1]
    height = jnp.broadcast_to(initial_height, (members,) + initial_height.shape)
    speeds = jnp.broadcast_to(initial_speed[:, None], (2, members) + initial_height.shape)
    for substep in range(STEPS):
        height, speeds = advance(height, speeds, parameters[0], parameters[1])
    return height


def predict(height, cells):
    flattened = height.reshape(height.shape[0], -1)
    wanted = cells.reshape(-1)
    picked = jnp.take(flattened, jnp.clip(wanted, 0, flattened.shape[1] - 1), axis=1)
    picked = jnp.where(wanted[None, :] >= 0, picked, jnp.float32(0.0))
    return picked.T.reshape(cells.shape[0], -1)


def gram_terms(predicted, observed, precision):
    members = predicted.shape[1]
    centre = jnp.mean(predicted, axis=1, keepdims=True)
    spread = predicted - centre
    weighted = spread * precision[:, None]
    misfit = observed[:, None] - predicted
    gram_part = jnp.dot(spread.T, weighted, precision=lax.Precision.HIGHEST) / members
    cross_part = jnp.dot(weighted.T, misfit, precision=lax.Precision.HIGHEST) / math.sqrt(members)
    return (gram_part, cross_part)


def solve_weights(gram_part, cross_part):
    members = gram_part.shape[0]
    system = jnp.eye(members, dtype=jnp.float32) + gram_part
    factor = jnp.linalg.cholesky(system)
    weights = jax.scipy.linalg.cho_solve((factor, True), cross_part) / math.sqrt(members)
    return weights - jnp.mean(weights, axis=0, keepdims=True)


def per_device_halo(parameters, initial_height, initial_speed, obs_slots, obs_values, obs_precision):
    owners = obs_slots.shape[2]
    slot_count = obs_slots.shape[3]
    members_here = parameters.shape[1]
    member_block = lax.axis_index("ens")
    owner_values, owner_precision = (
        lax.all_to_all(obs_values[:, 0], ("lat", "lon"), split_axis=1, concat_axis=1, tiled=True),
        lax.all_to_all(
            obs_precision[:, 0], ("lat", "lon"), split_axis=1, concat_axis=1, tiled=True
        ),
    )
    for iteration in range(ITERS):
        height = forward(parameters, initial_height, initial_speed)
        outgoing = predict(height, obs_slots[iteration, 0])
        received = outgoing
        observed = owner_values[iteration]
        precision = owner_precision[iteration]
        received = received.reshape(owners, slot_count, members_here)
        gathered = lax.all_gather(received, "ens", axis=2, tiled=True)
        members = gathered.shape[2]
        gram_part, cross_part = gram_terms(
            gathered.reshape(-1, members), observed.reshape(-1), precision.reshape(-1)
        )
        gram_part, cross_part = lax.psum((gram_part, cross_part), ("lat", "lon"))
        centred = solve_weights(gram_part, cross_part)
        local_weights = lax.dynamic_slice_in_dim(
            centred, member_block * members_here, members_here, 1
        )
        starting = jnp.zeros(
            (2, members_here, parameters.shape[2] * parameters.shape[3]), jnp.float32
        )
        pieces = lax.all_gather(parameters, "ens", axis=1, tiled=True)
        stacked = pieces.reshape(pieces.shape[0], pieces.shape[1], -1)
        increment = starting + jnp.einsum(
            "pjc,jm->pmc", stacked, local_weights, precision=lax.Precision.HIGHEST
        )
        parameters = parameters + increment.reshape(parameters.shape)
    return parameters


MESH = pl.DeviceIdType.MESH
VMEM = pltpu.VMEM


def east(field):
    width = field.shape[1]
    return pltpu.roll(field, width - 1, 1) - pltpu.roll(field, 1, 1)


def north(field, first_row, last_row):
    height = field.shape[0]
    after = jnp.where(last_row, 0.0, pltpu.roll(field, height - 1, 0))
    before = jnp.where(first_row, 0.0, pltpu.roll(field, 1, 0))
    return after - before


def run_member(height, speed_e, speed_n, friction, forcing):
    rows = lax.broadcasted_iota(jnp.int32, height.shape, 0)
    first_row, last_row = (rows == 0, rows == height.shape[0] - 1)
    keep = 1.0 - friction
    for substep in range(STEPS):
        flow = east(speed_e) + north(speed_n, first_row, last_row)
        height = height - depth_step * flow + forcing
        if substep < STEPS - 1:
            speed_e, speed_n = (
                keep * speed_e - gravity_step * east(height) + coriolis * speed_n,
                keep * speed_n
                - gravity_step * north(height, first_row, last_row)
                - coriolis * speed_e,
            )
    return height


def flat_line(block, width):
    depth, count = block.shape
    lanes = lax.broadcasted_iota(jnp.int32, (count, width), 1)
    slots = lax.broadcasted_iota(jnp.int32, (count, width), 0)
    spread_out = jnp.dot(
        block,
        (lax.rem(lanes, count) == slots).astype(jnp.float32),
        precision=lax.Precision.HIGHEST,
        preferred_element_type=jnp.float32,
    )
    owners = lax.broadcasted_iota(jnp.int32, (depth, width), 0)
    groups = lax.broadcasted_iota(jnp.int32, (depth, width), 1) // count
    return jnp.sum(jnp.where(owners == groups, spread_out, 0.0), axis=0, keepdims=True)


def gather_kernel(iteration, n_lat, n_lon, n_ens, *refs):
    first = iteration == 0
    blocks = n_lat * n_lon
    if first:
        params, start_height, start_speed, slots_in, values_in, precision_in = refs[:6]
        gram, cross, other, full, got, aux, send_a, recv_a, send_h, recv_h = refs[6:16]
        refs = refs[16:]
    else:
        params, full, gram, cross, other, got = refs[:6]
        refs = refs[6:]
    (held, load, outgoing, arrived, part, pieces, summed, total) = refs[:8]
    loading = pltpu.make_async_copy(params, held, load.at[0])
    loading.start()
    (send_p, recv_p, send_o, recv_o, send_y, recv_y, send_r, recv_r, send_t, recv_t) = refs[8:]
    lat, lon, ens = (lax.axis_index("lat"), lax.axis_index("lon"), lax.axis_index("ens"))
    me = lat * n_lon + lon
    here = ens * blocks + me
    everyone = blocks * n_ens
    mine = params.shape[1] // blocks
    rows, cols = params.shape[2:]

    def peer(block):
        return {"lat": block // n_lon, "lon": lax.rem(block, n_lon), "ens": ens}

    def anyone(flat):
        block = lax.rem(flat, blocks)
        return {"lat": block // n_lon, "lon": lax.rem(block, n_lon), "ens": flat // blocks}

    def each(count, body):
        def step(i, carry):
            body(i)
            return carry

        lax.fori_loop(1, count, step, 0)

    def send(src, dst, send_sem, recv_sem, device):
        return pltpu.make_async_remote_copy(
            src_ref=src,
            dst_ref=dst,
            send_sem=send_sem,
            recv_sem=recv_sem,
            device_id=device,
            device_id_type=MESH,
        )

    barrier = pltpu.get_barrier_semaphore()

    def greet(i):
        pl.semaphore_signal(
            barrier, inc=1, device_id=anyone(lax.rem(here + i, everyone)), device_id_type=MESH
        )

    each(everyone, greet)
    if first:
        lines = []
        for ref in (slots_in, values_in, precision_in):
            for t in range(ITERS):
                lines.append(flat_line(ref[t, 0].astype(jnp.float32), cols))
        lines.append(jnp.zeros((rows - len(lines), cols), jnp.float32))
        aux[0] = start_height[...]
        aux[1] = start_speed[0]
        aux[2] = start_speed[1]
        aux[3] = jnp.concatenate(lines, axis=0)
    pl.semaphore_wait(barrier, everyone - 1)
    loading.wait()

    partner = {"lat": lat, "lon": lon, "ens": 1 - ens}
    half = pl.ds(2 * ens, 2)

    def param_copy(j, i):
        to = lax.rem(me + i, blocks)
        return send(
            held.at[:, to * mine + j], got.at[me, j], send_p.at[j, i], recv_p.at[j, i], peer(to)
        )

    def aux_copy(i):
        to = lax.rem(me + i, blocks)
        return send(aux.at[half], full.at[me, half], send_a.at[i], recv_a.at[i], peer(to))

    def relay_copy():
        return send(full.at[:, half], full.at[:, half], send_h.at[0], recv_h.at[0], partner)

    if first:
        each(blocks, lambda i: aux_copy(i).start())
    for j in range(mine):
        each(blocks, functools.partial(lambda j, i: param_copy(j, i).start(), j))

    def swap_copy(i):
        return send(
            held, other.at[0], send_o.at[0], recv_o.at[0], partner
        )

    if first:
        full[me, half] = aux[half]
        each(blocks, lambda i: aux_copy(i).wait())
        relay_copy().start()
    swap_copy(0).start()
    for j in range(mine):
        got[me, j] = held[:, me * mine + j]
    if first:
        relay_copy().wait()

    def whole(pick):
        lines = []
        for a in range(n_lat):
            lines.append(jnp.concatenate([pick(a * n_lon + b) for b in range(n_lon)], axis=1))
        return jnp.concatenate(lines, axis=0)

    row_ids = lax.broadcasted_iota(jnp.int32, (rows, cols), 0)

    def member(j, carry):
        each(blocks, lambda i: param_copy(j, i).wait())
        height = run_member(
            whole(lambda b: full[b, 0]),
            whole(lambda b: full[b, 1]),
            whole(lambda b: full[b, 2]),
            whole(lambda b: got[b, j, 0]),
            whole(lambda b: got[b, j, 1]),
        )
        for b in range(blocks):
            cells = full[b, 3][iteration : iteration + 1].astype(jnp.int32)
            cells = jnp.broadcast_to(cells, (rows, cols))
            lanes = jnp.bitwise_and(cells, cols - 1)
            hit = row_ids == jnp.right_shift(cells, cols.bit_length() - 1)
            top, edge = ((b // n_lon) * rows, (b % n_lon) * cols)
            tile = height[top : top + rows, edge : edge + cols]
            found = jnp.where(hit, jnp.take_along_axis(tile, lanes, axis=1), 0.0)
            outgoing[b, pl.ds(j, 1)] = jnp.sum(found, axis=0, keepdims=True)
        return carry

    lax.fori_loop(0, mine, member, 0)

    def answer_copy(i):
        to = lax.rem(here + i, everyone)
        return send(
            outgoing.at[lax.rem(to, blocks)],
            arrived.at[here],
            send_y.at[i],
            recv_y.at[i],
            anyone(to),
        )

    each(everyone, lambda i: answer_copy(i).start())
    arrived[here] = outgoing[me]

    slots = full.shape[-1] // blocks
    heard = jnp.concatenate([full[b, 3] for b in range(blocks)], axis=0)
    kinds = full.shape[2]
    lane_ids = lax.broadcasted_iota(jnp.int32, heard.shape, 1)
    line_ids = lax.broadcasted_iota(jnp.int32, heard.shape, 0)
    square = (heard.shape[1], heard.shape[1])
    from_ids = lax.broadcasted_iota(jnp.int32, square, 0)
    to_ids = lax.broadcasted_iota(jnp.int32, square, 1)
    chosen = from_ids == me * slots + lax.rem(to_ids, slots)
    spread_out = jnp.dot(
        heard,
        chosen.astype(jnp.float32),
        precision=lax.Precision.HIGHEST,
        preferred_element_type=jnp.float32,
    )

    def of_kind(kind):
        wanted = line_ids == (lane_ids // slots) * kinds + kind
        return jnp.sum(jnp.where(wanted, spread_out, 0.0), axis=0, keepdims=True)

    observed = of_kind(2 + iteration)
    precision = of_kind(4 + iteration)

    each(everyone, lambda i: answer_copy(i).wait())

    predicted = jnp.concatenate([arrived[s] for s in range(everyone)], axis=0)
    members = predicted.shape[0]
    spread = predicted - jnp.sum(predicted, axis=0, keepdims=True) / members
    weighted = spread * precision
    is_gram = ens == 0
    right = jnp.where(is_gram, spread, observed - predicted)
    scale = jnp.where(is_gram, 1.0 / members, 1.0 / math.sqrt(members))
    product = lax.dot_general(
        weighted,
        right,
        (((1,), (1,)), ((), ())),
        precision=lax.Precision.HIGHEST,
        preferred_element_type=jnp.float32,
    )
    product = product * scale
    lines = members // blocks
    for b in range(blocks):
        part[b] = product[b * lines : (b + 1) * lines]

    def piece_copy(i):
        to = lax.rem(me + i, blocks)
        return send(part.at[to], pieces.at[me], send_r.at[i], recv_r.at[i], peer(to))

    each(blocks, lambda i: piece_copy(i).start())
    pieces[me] = part[me]
    each(blocks, lambda i: piece_copy(i).wait())
    line = pieces[0]
    for b in range(1, blocks):
        line = line + pieces[b]
    summed[...] = line

    def total_copy(i):
        to = lax.rem(here + i, everyone)
        return send(summed, total.at[here], send_t.at[i], recv_t.at[i], anyone(to))

    each(everyone, lambda i: total_copy(i).start())
    total[here] = line
    each(everyone, lambda i: total_copy(i).wait())
    for b in range(blocks):
        gram[b * lines : (b + 1) * lines, :] = total[b]
        cross[b * lines : (b + 1) * lines, :] = total[blocks + b]
    swap_copy(0).wait()


def gather_call(iteration, sizes, params, *extra):
    n_lat, n_lon, n_ens = sizes
    blocks = n_lat * n_lon
    everyone = blocks * n_ens
    members_here, rows, cols = params.shape[1:]
    members = members_here * n_ens
    mine = members_here // blocks
    lines = members // blocks
    f32 = jnp.float32
    dma = pltpu.SemaphoreType.DMA
    first = iteration == 0
    outs = [
        jax.ShapeDtypeStruct((members, members), f32),
        jax.ShapeDtypeStruct((members, members), f32),
        jax.ShapeDtypeStruct((1,) + params.shape, f32),
    ]
    scratch = [
        VMEM((blocks, mine, 2, rows, cols), f32),
    ]
    if first:
        outs.append(jax.ShapeDtypeStruct((blocks, 4, rows, cols), f32))
        scratch.append(VMEM((4, rows, cols), f32))
        scratch += [dma((blocks,)), dma((blocks,)), dma((1,)), dma((1,))]
    scratch += [
        VMEM(params.shape, f32),
        dma((1,)),
        VMEM((blocks, mine, cols), f32),
        VMEM((everyone, mine, cols), f32),
        VMEM((blocks, lines, members), f32),
        VMEM((blocks, lines, members), f32),
        VMEM((lines, members), f32),
        VMEM((everyone, lines, members), f32),
        dma((mine, blocks)),
        dma((mine, blocks)),
        dma((1,)),
        dma((1,)),
        dma((everyone,)),
        dma((everyone,)),
        dma((blocks,)),
        dma((blocks,)),
        dma((everyone,)),
        dma((everyone,)),
    ]
    near, far = (pl.BlockSpec(memory_space=space) for space in (VMEM, pl.ANY))
    return pl.pallas_call(
        functools.partial(gather_kernel, iteration, n_lat, n_lon, n_ens),
        out_shape=outs,
        in_specs=[far] + [near] * len(extra),
        out_specs=[near, near, far] + [near] * (len(outs) - 3),
        scratch_shapes=scratch,
        compiler_params=pltpu.CompilerParams(
            collective_id=iteration, has_side_effects=True, vmem_limit_bytes=40 * 2**20
        ),
    )(params, *extra)


def with_rows(value, rows, start):
    end = start + rows.shape[0]
    pieces = [value[:start]] if start else []
    pieces.append(rows)
    if end < value.shape[0]:
        pieces.append(value[end:])
    return jnp.concatenate(pieces, axis=0)


def eliminate(left, right):
    size = left.shape[0]
    panel = 8
    row_ids = lax.broadcasted_iota(jnp.int32, (panel, size), 0)
    for start in range(0, size, panel):
        end = start + panel
        rows_left, rows_right = (left[start:end], right[start:end])
        columns = [
            jnp.broadcast_to(rows_left[:, start + k : start + k + 1], (panel, size))
            for k in range(panel)
        ]
        for k in range(panel):
            column = columns[k]
            inverse = 1.0 / column[k : k + 1]
            here = row_ids == k

            def reduce(value):
                pivot_row = value[k : k + 1] * inverse
                return jnp.where(here, pivot_row, value - column * pivot_row)

            rows_left, rows_right = (reduce(rows_left), reduce(rows_right))
            for later in range(k + 1, panel):
                columns[later] = reduce(columns[later])
        next_left, next_right = (left, right)
        for k in range(panel):
            column = left[:, start + k : start + k + 1]
            next_left = next_left - column * rows_left[k : k + 1]
            next_right = next_right - column * rows_right[k : k + 1]
        left = with_rows(next_left, rows_left, start)
        right = with_rows(next_right, rows_right, start)
    return right


def update_kernel(gram, cross, params, other, out):
    ens = lax.axis_index("ens")
    members = gram.shape[0]
    members_here = params.shape[1]
    ids = [lax.broadcasted_iota(jnp.int32, gram.shape, axis) for axis in (0, 1)]
    system = gram[...] + (ids[0] == ids[1]).astype(jnp.float32)
    weights = eliminate(system, cross[...]) / math.sqrt(members)
    centred = weights - jnp.sum(weights, axis=0, keepdims=True) / members
    turned = centred.T
    mine = jnp.where(ens == 0, turned[:members_here], turned[members_here:])
    mine = jnp.where(ens == 0, mine, pltpu.roll(mine, members_here, 1))
    for p in range(params.shape[0]):
        for r in range(params.shape[2]):
            local = params[p, :, r, :]
            stacked = jnp.concatenate([local, other[0, p, :, r, :]], axis=0)
            out[p, :, r, :] = local + jnp.dot(
                mine,
                stacked,
                precision=lax.Precision.HIGHEST,
                preferred_element_type=jnp.float32,
            )


def update_call(gram, cross, params, other):
    return pl.pallas_call(
        update_kernel,
        out_shape=jax.ShapeDtypeStruct(params.shape, jnp.float32),
        in_specs=[pl.BlockSpec(memory_space=VMEM)] * 4,
        out_specs=pl.BlockSpec(memory_space=VMEM),
        compiler_params=pltpu.CompilerParams(vmem_limit_bytes=40 * 2**20),
    )(gram, cross, params, other)


def per_device_members(
    sizes, parameters, initial_height, initial_speed, obs_slots, obs_values, obs_precision
):
    observations = (obs_slots, obs_values, obs_precision)
    gram, cross, other, full = gather_call(
        0, sizes, parameters, initial_height, initial_speed, *observations
    )
    parameters = update_call(gram, cross, parameters, other)
    for iteration in range(1, ITERS):
        gram, cross, other = gather_call(iteration, sizes, parameters, full)
        parameters = update_call(gram, cross, parameters, other)
    return parameters


def by_members(sizes, parameters, initial_height, initial_speed, obs_slots, *rest):
    n_lat, n_lon, n_ens = sizes
    blocks = n_lat * n_lon
    members_here, rows, cols = parameters.shape[1:]
    fits = (
        n_ens == 2
        and members_here % blocks == 0
        and members_here // blocks <= rows
        and rows == 8
        and members_here * n_ens == blocks * 8
        and cols == 128
        and obs_slots.shape[2] * obs_slots.shape[3] == cols
    )
    arguments = (parameters, initial_height, initial_speed, obs_slots) + rest
    if fits:
        return per_device_members(sizes, *arguments)
    return per_device_halo(*arguments)


def solution(mesh):
    placed = (
        P(None, "ens", "lat", "lon"),
        P("lat", "lon"),
        P(None, "lat", "lon"),
        P(None, ("lat", "lon"), None, None),
        P(None, ("lat", "lon"), None, None),
        P(None, ("lat", "lon"), None, None),
    )
    return jax.shard_map(
        functools.partial(by_members, tuple(mesh.shape[a] for a in ("lat", "lon", "ens"))),
        mesh=mesh,
        in_specs=placed,
        out_specs=P(None, "ens", "lat", "lon"),
        check_vma=False,
    )
```
